128 devices in a mesh: rep: 1, dp: 16 (over z, y), ad: 8 (over x, core).
Axes of the slice: x: 4, y: 4, z: 4, core: 2. Of those that a mesh axis runs over, the one named last changes fastest.
Arguments:
- x_rows: bfloat16 [65536, 3072], P(('rep', 'dp', 'ad'))
- adapter_id: int32 [65536], P(('rep', 'dp', 'ad'))
- w_gate: bfloat16 [3072, 8192], replicated
- w_up: bfloat16 [3072, 8192], replicated
- w_down: bfloat16 [8192, 3072], replicated
- a_gate: bfloat16 [16, 3072, 32], P('ad')
- b_gate: bfloat16 [16, 32, 8192], P('ad')
- a_up: bfloat16 [16, 3072, 32], P('ad')
- b_up: bfloat16 [16, 32, 8192], P('ad')
- a_down: bfloat16 [16, 8192, 32], P('ad')
- b_down: bfloat16 [16, 32, 3072], P('ad')
Outputs:
- output: bfloat16 [65536, 3072], P(('rep', 'dp', 'ad'))
All inputs are finite; a program needn't handle non-finite values.
Results may differ from the reference program's by a relative error of at most 0.00131.
Values are sent between devices in bfloat16 or wider.
A program may use at most 1 GiB of HBM per device.

```python
import jax
import jax.numpy as jnp
from jax import lax

D_MODEL = 3072
D_FF = 8192
RANK = 32
LORA_ALPHA = 32
TOKENS_DEV = 512
GROUP = 8
REPLICAS = 16
ADAPTERS = 16
ROW_BLOCK = 32
SOURCES = REPLICAS * GROUP
TOKENS = SOURCES * TOKENS_DEV
ADAPT_LOCAL = ADAPTERS // GROUP
CAPACITY = (TOKENS_DEV // GROUP) * min(4, max(1, GROUP // 2))


def draw_adapter_ids(key_ids):
    key_hot, key_off, key_perm, key_tok = jax.random.split(key_ids, 4)
    hot_base = jax.random.randint(key_hot, (), 0, GROUP)
    offset = jax.random.randint(key_off, (), 0, ADAPT_LOCAL)
    labels = jax.random.permutation(key_perm, ADAPT_LOCAL)
    source = jnp.arange(SOURCES)
    hot_owner = (hot_base + source // GROUP) % GROUP
    distance = (jnp.arange(GROUP)[None, :] - hot_owner[:, None]) % GROUP
    rest = TOKENS_DEV - CAPACITY
    cold_base = rest // (GROUP - 1)
    cold_extra = rest % (GROUP - 1)
    counts = jnp.where(distance == 0, CAPACITY, cold_base + (distance - 1 < cold_extra).astype(jnp.int32))
    owner_sorted = jax.vmap(lambda count_row: jnp.repeat(jnp.arange(GROUP), count_row, total_repeat_length=TOKENS_DEV))(counts)
    starts = jnp.cumsum(counts, axis=1) - counts
    within = jnp.arange(TOKENS_DEV)[None, :] - jnp.take_along_axis(starts, owner_sorted, axis=1)
    spread = within * SOURCES + source[:, None] + offset
    ids_sorted = owner_sorted * ADAPT_LOCAL + labels[spread % ADAPT_LOCAL]
    orders = jax.vmap(lambda sub_key: jax.random.permutation(sub_key, TOKENS_DEV))(jax.random.split(key_tok, SOURCES))
    return jnp.take_along_axis(ids_sorted, orders, axis=1).reshape(-1).astype(jnp.int32)


def setup_inputs(seed: int = 0, part: int = 0) -> dict:
    key_part = jax.random.fold_in(jax.random.key(seed), part)
    key_x, key_ids = jax.random.split(key_part)
    keys = jax.random.split(jax.random.key(seed + 1), 9)
    scale = LORA_ALPHA / RANK
    up_std = 0.4 / (scale * RANK ** 0.5)
    down_std = 0.5 / (scale * RANK ** 0.5)

    def normal(sub_key, shape, std_dev):
        return (jax.random.normal(sub_key, shape, jnp.float32) * std_dev).astype(jnp.bfloat16)

    return {
        "x_rows": normal(key_x, (TOKENS, D_MODEL), 1.0),
        "adapter_id": draw_adapter_ids(key_ids),
        "w_gate": normal(keys[0], (D_MODEL, D_FF), D_MODEL ** -0.5),
        "w_up": normal(keys[1], (D_MODEL, D_FF), D_MODEL ** -0.5),
        "w_down": normal(keys[2], (D_FF, D_MODEL), D_FF ** -0.5),
        "a_gate": normal(keys[3], (ADAPTERS, D_MODEL, RANK), D_MODEL ** -0.5),
        "b_gate": normal(keys[4], (ADAPTERS, RANK, D_FF), up_std),
        "a_up": normal(keys[5], (ADAPTERS, D_MODEL, RANK), D_MODEL ** -0.5),
        "b_up": normal(keys[6], (ADAPTERS, RANK, D_FF), up_std),
        "a_down": normal(keys[7], (ADAPTERS, D_FF, RANK), D_FF ** -0.5),
        "b_down": normal(keys[8], (ADAPTERS, RANK, D_MODEL), down_std),
    }


def reference(x_rows, adapter_id, w_gate, w_up, w_down, a_gate, b_gate, a_up, b_up, a_down, b_down):
    scale = LORA_ALPHA / RANK
    n_blocks = TOKENS // ROW_BLOCK

    def low_rank(rows_in, block_ids, a_mat, b_mat):
        a_sel = jnp.take(a_mat, block_ids, axis=0).astype(jnp.float32)
        low_proj = jnp.einsum("tk,tkr->tr", rows_in.astype(jnp.float32), a_sel).astype(jnp.bfloat16)
        b_sel = jnp.take(b_mat, block_ids, axis=0).astype(jnp.float32)
        wide_proj = jnp.einsum("tr,trn->tn", low_proj.astype(jnp.float32), b_sel)
        return (scale * wide_proj).astype(jnp.bfloat16).astype(jnp.float32)

    def one_block(block):
        x_blk, block_ids = block
        gate_pre = jnp.dot(x_blk, w_gate, preferred_element_type=jnp.float32) + low_rank(x_blk, block_ids, a_gate, b_gate)
        up_proj = jnp.dot(x_blk, w_up, preferred_element_type=jnp.float32) + low_rank(x_blk, block_ids, a_up, b_up)
        hidden = (jax.nn.silu(gate_pre) * up_proj).astype(jnp.bfloat16)
        down_proj = jnp.dot(hidden, w_down, preferred_element_type=jnp.float32) + low_rank(hidden, block_ids, a_down, b_down)
        return (x_blk.astype(jnp.float32) + down_proj).astype(jnp.bfloat16)

    result = lax.map(one_block, (x_rows.reshape(n_blocks, ROW_BLOCK, D_MODEL), adapter_id.reshape(n_blocks, ROW_BLOCK)))
    return result.reshape(TOKENS, D_MODEL)
```

```python
import functools

import jax
import jax.numpy as jnp
from jax import lax
from jax.experimental import pallas as pl
from jax.experimental.pallas import tpu as pltpu
from jax.sharding import PartitionSpec as P

LORA_ALPHA = 32
MESH = pl.DeviceIdType.MESH
CHUNK = 1024
TILE = 256
SLOTS = 4
PEND = 10
AHEAD = 3
LAGS = (1, 3, 5, 6)
RING = 4


def kernel(scale, rank, x_hbm, ids_ref, wg_hbm, wu_hbm, wd_hbm, ag_hbm, au_hbm, bg_hbm, bu_hbm, ad_hbm, bd_hbm,
           out_hbm, x_v, gath, hid, low, load_sem, r1, r2, r3, r5, r7, send_sem, wsem, xsem, osem):
    rows, d_model = x_v.shape
    d_ff = hid.shape[1]
    n_chunks, n_rank, _ = gath.shape
    own_rows = ag_hbm.shape[0]
    half, quarter = own_rows // 2, own_rows // 4
    n_a = 2 * d_model // CHUNK
    n_b = 2 * d_ff // CHUNK
    n_d = d_ff // CHUNK
    n_tiles = d_ff // TILE
    n_out = d_model // TILE
    hc = CHUNK // 2

    dp = lax.axis_index("dp")
    ad = lax.axis_index("ad")
    x, core = ad // 2, ad % 2
    z, y = dp // RING, dp % RING
    par = y % 2
    xp = {"dp": dp, "ad": ((x + 1) % RING) * 2 + core}
    xm = {"dp": dp, "ad": ((x + RING - 1) % RING) * 2 + core}
    yp = {"dp": z * RING + (y + 1) % RING, "ad": ad}
    ym = {"dp": z * RING + (y + RING - 1) % RING, "ad": ad}
    sib = {"dp": dp, "ad": x * 2 + (1 - core)}

    def row_of(owner_x):
        return (owner_x * 2 + core) * own_rows

    r_own = row_of(x)
    r_m = row_of((x + RING - 1) % RING)
    r_p = row_of((x + 1) % RING)
    r_o = row_of((x + 2) % RING)
    mine = par * half
    other = (1 - par) * half

    def looped(n, fn):
        lax.fori_loop(0, n, lambda i, c: (fn(i), c)[1], 0)

    def up_loads(ring, t, slot):
        cols = pl.ds(pl.multiple_of(t * TILE, TILE), TILE)
        pltpu.make_async_copy(wg_hbm.at[:, cols], ring.at[slot], wsem.at[slot]).start()
        pltpu.make_async_copy(wu_hbm.at[:, cols], ring.at[slot + 1], wsem.at[slot + 1]).start()

    def up_wait(ring, slot):
        pltpu.make_async_copy(wg_hbm.at[:, pl.ds(0, TILE)], ring.at[slot], wsem.at[slot]).wait()

    def wide(low_rows, b_all):
        return (scale * jnp.dot(low_rows, b_all, preferred_element_type=jnp.float32)).astype(jnp.bfloat16).astype(
            jnp.float32)

    def select(proj):
        col = lax.broadcasted_iota(jnp.int32, proj.shape, 1) // rank
        keep = ids_ref[...] == col
        return jnp.where(keep, proj, 0.0).astype(jnp.bfloat16)

    def dot_nt(lhs, rhs):
        return lax.dot_general(lhs, rhs, (((1,), (1,)), ((), ())), preferred_element_type=jnp.float32)

    def phase1(ring, pend):
        barrier = pltpu.get_barrier_semaphore()
        for dev in (xp, xm, yp, ym, sib):
            pl.semaphore_signal(barrier, inc=1, device_id=dev, device_id_type=MESH)

        x_copy = pltpu.make_async_copy(x_hbm, x_v, xsem.at[0])
        x_copy.start()

        def span(c, row, n):
            return gath.at[c, pl.ds(pl.multiple_of(row, quarter), n), :]

        up_loads(ring, 0, 0)
        own = pl.ds(pl.multiple_of(r_own, own_rows), own_rows)

        def load_pair(c, k, first, second):
            cols = pl.ds(pl.multiple_of(k * hc, hc), hc)
            pltpu.make_async_copy(first.at[:, cols], gath.at[c, own, pl.ds(0, hc)], load_sem.at[c]).start()
            pltpu.make_async_copy(second.at[:, cols], gath.at[c, own, pl.ds(hc, hc)], load_sem.at[c]).start()

        def load_one(c, k, src):
            cols = pl.ds(pl.multiple_of(k * CHUNK, CHUNK), CHUNK)
            pltpu.make_async_copy(src.at[:, cols], gath.at[c, own, :], load_sem.at[c]).start()

        looped(n_a, lambda k: load_pair(k, k, ag_hbm, au_hbm))
        up_loads(ring, 1, 2)
        looped(n_b, lambda k: load_pair(n_a + k, k, bg_hbm, bu_hbm))
        looped(n_d, lambda k: load_one(n_a + n_b + k, k, ad_hbm))
        looped(n_chunks - n_a - n_b - n_d, lambda k: load_one(n_a + n_b + n_d + k, k, bd_hbm))

        def rcopy(c, row, n, sem, dev):
            return pltpu.make_async_remote_copy(src_ref=span(c, row, n), dst_ref=span(c, row, n), send_sem=send_sem.at[c],
                                                recv_sem=sem.at[c], device_id=dev, device_id_type=MESH)

        def send(c, row, n, sem, dev):
            rcopy(c, row, n, sem, dev).start()

        def arrived(c, n, sem):
            rcopy(c, 0, n, sem, sib).wait_recv()

        def stage0(c):
            pltpu.make_async_copy(bd_hbm.at[:, pl.ds(0, CHUNK)], gath.at[c, own, :], load_sem.at[c]).wait()
            send(c, r_own + mine, half, r1, xp)
            send(c, r_own + mine, half, r2, xm)
            send(c, r_own, own_rows, r7, sib)

        def stage1(c):
            arrived(c, half, r1)
            arrived(c, half, r2)
            send(c, r_m + mine, quarter, r3, xp)
            send(c, r_p + mine + quarter, quarter, r3, xm)
            for r in (r_m, r_p):
                send(c, r + mine, quarter, r5, yp)
                send(c, r + mine + quarter, quarter, r5, ym)
                send(c, r + mine, half, r7, sib)

        def stage2(c):
            arrived(c, half, r3)
            send(c, r_o + mine, quarter, r5, yp)
            send(c, r_o + mine + quarter, quarter, r5, ym)
            send(c, r_o + mine, half, r7, sib)

        def stage3(c):
            arrived(c, 3 * half, r5)
            for r in (r_m, r_p, r_o):
                send(c, r + other, half, r7, sib)

        def stage4(c):
            arrived(c, RING * own_rows, r7)

        def step(n):
            for c, fn in ((n + AHEAD, stage0), (n - LAGS[0], stage1), (n - LAGS[1], stage2), (n - LAGS[2], stage3),
                          (n - LAGS[3], stage4)):
                pl.when(jnp.logical_and(c >= 0, c < n_chunks))(functools.partial(fn, c))

        pl.semaphore_wait(barrier, 5)
        for c in range(AHEAD):
            stage0(c)
        x_copy.wait()

        def base(t):
            slot = 2 * (t % 2)
            at = t % PEND
            pend[at, 0] = jnp.dot(x_v[...], ring[slot], preferred_element_type=jnp.float32)
            pend[at, 1] = jnp.dot(x_v[...], ring[slot + 1], preferred_element_type=jnp.float32)

        def take(t):
            slot = 2 * (t % 2)
            up_wait(ring, slot)
            up_wait(ring, slot + 1)

        def refill(t):
            @pl.when(t + 2 < n_tiles)
            def _():
                up_loads(ring, t + 2, 2 * (t % 2))

        per = hc // TILE

        def finish(t):
            c = n_a + t // per
            off = pl.multiple_of((t % per) * TILE, TILE)
            at = t % PEND
            gate = pend[at, 0] + wide(low[0], gath[c, :, pl.ds(off, TILE)])
            up = pend[at, 1] + wide(low[1], gath[c, :, pl.ds(pl.multiple_of(hc + off, TILE), TILE)])
            hid[:, pl.ds(pl.multiple_of(t * TILE, TILE), TILE)] = (jax.nn.silu(gate) * up).astype(jnp.bfloat16)

        def first_loop(n):
            step(n)
            take(n)
            base(n)
            refill(n)

        looped(PEND, first_loop)

        for i in range(PEND, n_a + LAGS[3]):
            pl.when(i >= PEND)(functools.partial(step, jnp.int32(i)))
        extra = max(PEND, n_a + LAGS[3]) - PEND

        for kind in range(2):
            acc = None
            for k in range(n_a):
                part = dot_nt(x_v[:, k * hc:(k + 1) * hc], gath[k, :, kind * hc:(kind + 1) * hc])
                acc = part if acc is None else acc + part
            low[kind] = select(acc)

        def second_loop(i):
            n = i + PEND
            step(n + extra)
            take(n)
            finish(n - PEND)
            base(n)
            refill(n)

        looped(n_tiles - PEND, second_loop)
        def third_loop(i):
            n = i + n_tiles
            step(n + extra)
            finish(n - PEND)

        looped(PEND, third_loop)
        for i in range(n_tiles + PEND + extra, n_chunks + LAGS[3]):
            step(jnp.int32(i))

    pl.run_scoped(phase1, pltpu.VMEM((SLOTS, d_model, TILE), jnp.bfloat16),
                  pltpu.VMEM((PEND, 2, rows, TILE), jnp.float32))

    def phase2(wd_v, acc):
        def down_copy(n):
            cols = pl.ds(pl.multiple_of(n * TILE, TILE), TILE)
            return pltpu.make_async_copy(wd_hbm.at[:, cols], wd_v.at[n % 2], wsem.at[n % 2])

        down_copy(0).start()
        down_copy(1).start()
        acc[...] = jnp.zeros_like(acc)

        def low_down(k):
            lhs = hid[:, pl.ds(pl.multiple_of(k * CHUNK, CHUNK), CHUNK)]
            acc[...] += dot_nt(lhs, gath[n_a + n_b + k])

        looped(n_d, low_down)
        low[0] = select(acc[...])
        per_e = CHUNK // TILE

        def out_copy(n):
            cols = pl.ds(pl.multiple_of(n * TILE, TILE), TILE)
            return pltpu.make_async_copy(x_v.at[:, cols], out_hbm.at[:, cols], osem.at[n])

        def down(n):
            down_copy(n).wait()
            cols = pl.ds(pl.multiple_of(n * TILE, TILE), TILE)
            off = pl.multiple_of((n % per_e) * TILE, TILE)
            delta = wide(low[0], gath[n_a + n_b + n_d + n // per_e, :, pl.ds(off, TILE)])
            total = jnp.dot(hid[...], wd_v[n % 2], preferred_element_type=jnp.float32) + delta
            x_v[:, cols] = (x_v[:, cols].astype(jnp.float32) + total).astype(jnp.bfloat16)
            out_copy(n).start()

            @pl.when(n + 2 < n_out)
            def _():
                down_copy(n + 2).start()

        looped(n_out, down)
        looped(n_out, lambda n: out_copy(n).wait())
        sent = 7 * own_rows
        looped(n_chunks, lambda c: pltpu.make_async_remote_copy(
            src_ref=gath.at[c, pl.ds(0, sent), :], dst_ref=gath.at[c, pl.ds(0, sent), :], send_sem=send_sem.at[c],
            recv_sem=r7.at[c], device_id=sib, device_id_type=MESH).wait_send())

    pl.run_scoped(phase2, pltpu.VMEM((2, d_ff, TILE), jnp.bfloat16), pltpu.VMEM((rows, n_rank), jnp.float32))


def solution(mesh):
    group = mesh.shape["ad"]
    tok_axes = ("rep", "dp", "ad")
    row_spec = P(tok_axes, None)
    owned = P("ad", None, None)

    def local_step(x_rows, adapter_id, w_gate, w_up, w_down, a_gate, b_gate, a_up, b_up, a_down, b_down):
        n_rows, d_model = x_rows.shape
        d_ff = w_gate.shape[1]
        n_local, _, rank = a_gate.shape
        local = n_local * rank
        n_rank = group * local
        n_chunks = (3 * d_model + 3 * d_ff) // CHUNK

        def cols_of(mat):
            return mat.transpose(0, 2, 1).reshape(local, mat.shape[1])

        def rows_of(mat):
            return mat.reshape(local, mat.shape[2])

        dma = lambda n: pltpu.SemaphoreType.DMA((n,))
        anyspec = pl.BlockSpec(memory_space=pl.ANY)
        flops = 2 * n_rows * (3 * d_model * d_ff + n_rank * (3 * d_model + 3 * d_ff))
        call = pl.pallas_call(
            functools.partial(kernel, LORA_ALPHA / rank, rank),
            out_shape=jax.ShapeDtypeStruct((n_rows, d_model), x_rows.dtype),
            in_specs=[anyspec, pl.BlockSpec(memory_space=pltpu.VMEM)] + [anyspec] * 9,
            out_specs=anyspec,
            scratch_shapes=[
                pltpu.VMEM((n_rows, d_model), jnp.bfloat16),
                pltpu.VMEM((n_chunks, n_rank, CHUNK), jnp.bfloat16),
                pltpu.VMEM((n_rows, d_ff), jnp.bfloat16),
                pltpu.VMEM((2, n_rows, n_rank), jnp.bfloat16),
                dma(n_chunks), dma(n_chunks), dma(n_chunks), dma(n_chunks), dma(n_chunks), dma(n_chunks),
                dma(n_chunks), dma(SLOTS), dma(1), dma(d_model // TILE),
            ],
            compiler_params=pltpu.CompilerParams(collective_id=0, has_side_effects=True, vmem_limit_bytes=67043328),
            cost_estimate=pl.CostEstimate(flops=flops, bytes_accessed=6 * d_model * d_ff, transcendentals=n_rows * d_ff),
            name="lora_mlp",
        )
        return call(x_rows, adapter_id.reshape(n_rows, 1), w_gate, w_up, w_down, cols_of(a_gate), cols_of(a_up),
                    rows_of(b_gate), rows_of(b_up), cols_of(a_down), rows_of(b_down))

    return jax.shard_map(local_step, mesh=mesh,
                         in_specs=(row_spec, P(tok_axes), P(), P(), P(), owned, owned, owned, owned, owned, owned),
                         out_specs=row_spec, check_vma=False)
```
